32 devices in a mesh: dp: 2 (over x), sp: 16 (over z, y, core).
Axes of the slice: x: 2, y: 2, z: 4, core: 2. Of those that a mesh axis runs over, the one named last changes fastest.
Arguments:
- x: bfloat16 [4, 16384, 2048], P('dp', 'sp'), parts along dimension 0
- w_q: bfloat16 [2048, 8, 256], replicated
- w_k: bfloat16 [2048, 8, 256], replicated
- w_v: bfloat16 [2048, 8, 256], replicated
- w_o: bfloat16 [8, 256, 2048], replicated
Outputs:
- output: bfloat16 [4, 16384, 2048], P('dp', 'sp'), parts along dimension 0
There are 2 independent parts. The reference program is written for one: setup_inputs(seed, part) draws one part's arguments, and reference() takes and returns one part's arrays. A program takes and returns all parts, laid end to end along the dimension named above; an argument that names none is the same for every part.
All inputs are finite; a program needn't handle non-finite values.
Results may differ from the reference program's by a relative error of at most 0.00355872.
Values are sent between devices in bfloat16 or wider.
A program may use at most 1 GiB of HBM per device.

```python
import jax
import jax.numpy as jnp
from jax import lax

MODEL_DIM = 2048
NUM_HEADS = 8
HEAD_DIM = 256
SEQ_LEN = 16384
NUM_SEQS = 2
SEGMENT = 2048
BRANCHES = 4
QUERY_BLOCK = 128


def setup_inputs(seed: int = 0, part: int = 0) -> dict:
    root_key = jax.random.key(seed)
    key_x = jax.random.fold_in(jax.random.fold_in(root_key, 1), part)
    key_q, key_k, key_v, key_o = jax.random.split(jax.random.fold_in(root_key, 2), 4)
    in_scale = MODEL_DIM ** -0.5
    out_scale = (NUM_HEADS * HEAD_DIM) ** -0.5
    w_shape = (MODEL_DIM, NUM_HEADS, HEAD_DIM)
    x = jax.random.normal(key_x, (NUM_SEQS, SEQ_LEN, MODEL_DIM), jnp.float32)
    w_q = jax.random.normal(key_q, w_shape, jnp.float32) * (1.4 * in_scale)
    w_k = jax.random.normal(key_k, w_shape, jnp.float32) * (1.4 * in_scale)
    w_v = jax.random.normal(key_v, w_shape, jnp.float32) * in_scale
    w_o = jax.random.normal(key_o, (NUM_HEADS, HEAD_DIM, MODEL_DIM), jnp.float32) * (8.0 * out_scale)
    return {'x': x.astype(jnp.bfloat16), 'w_q': w_q.astype(jnp.bfloat16), 'w_k': w_k.astype(jnp.bfloat16), 'w_v': w_v.astype(jnp.bfloat16), 'w_o': w_o.astype(jnp.bfloat16)}


def pick_rows(values, dilation):
    n_rows, n_heads, head_dim = values.shape
    split_view = values.reshape(n_rows // dilation, dilation, n_heads // dilation, dilation, head_dim)
    picked = jnp.stack([split_view[:, phase_idx, :, phase_idx, :] for phase_idx in range(dilation)], axis=2)
    return picked.reshape(n_rows // dilation, n_heads, head_dim)


def spread_rows(o_sp, lse_sp, dilation):
    n_rows, n_heads, head_dim = o_sp.shape
    keep_mask = jnp.eye(dilation, dtype=jnp.float32).reshape(1, dilation, 1, dilation)
    o_full = o_sp.reshape(n_rows, 1, n_heads // dilation, dilation, head_dim) * keep_mask[:, :, :, :, None]
    lse_full = jnp.where(keep_mask > 0, lse_sp.reshape(n_rows, 1, n_heads // dilation, dilation), -jnp.inf)
    return o_full.reshape(n_rows * dilation, n_heads, head_dim), lse_full.reshape(n_rows * dilation, n_heads)


def attend(q_sp, k_sp, v_sp):
    n_groups, n_query, n_heads, head_dim = q_sp.shape
    blk_len = min(QUERY_BLOCK, n_query)
    n_blocks = n_query // blk_len
    q_blocks = q_sp.reshape(n_groups * n_blocks, blk_len, n_heads, head_dim)
    owners = jnp.arange(n_groups * n_blocks, dtype=jnp.int32) // n_blocks
    logit_scale = head_dim ** -0.5

    def one_block(block_item):
        q_tile, owner_idx = block_item
        k_seg = lax.dynamic_index_in_dim(k_sp, owner_idx, 0, keepdims=False).astype(jnp.float32)
        v_seg = lax.dynamic_index_in_dim(v_sp, owner_idx, 0, keepdims=False).astype(jnp.float32)
        scores = jnp.einsum('qhd,khd->hqk', q_tile.astype(jnp.float32), k_seg) * logit_scale
        log_sum = jax.nn.logsumexp(scores, axis=-1)
        p_tile = jnp.exp(scores - log_sum[:, :, None]).astype(jnp.bfloat16).astype(jnp.float32)
        o_tile = jnp.einsum('hqk,khd->qhd', p_tile, v_seg)
        return o_tile, log_sum.T

    o_all, lse_all = lax.map(one_block, (q_blocks, owners))
    return o_all.reshape(n_groups * n_query, n_heads, head_dim), lse_all.reshape(n_groups * n_query, n_heads)


def reference(x, w_q, w_k, w_v, w_o):
    def project(x_seq, weight):
        product = jnp.dot(x_seq, weight.reshape(MODEL_DIM, NUM_HEADS * HEAD_DIM), preferred_element_type=jnp.float32)
        return product.astype(jnp.bfloat16).reshape(SEQ_LEN, NUM_HEADS, HEAD_DIM)

    def one_sequence(x_seq):
        q_all = project(x_seq, w_q)
        k_all = project(x_seq, w_k)
        v_all = project(x_seq, w_v)
        branch_outs = []
        branch_lse = []
        for branch in range(BRANCHES):
            dilation = 2 ** branch
            n_seg = SEQ_LEN // (SEGMENT * dilation)
            seg_shape = (n_seg, SEGMENT, NUM_HEADS, HEAD_DIM)
            o_sp, lse_sp = attend(pick_rows(q_all, dilation).reshape(seg_shape), pick_rows(k_all, dilation).reshape(seg_shape), pick_rows(v_all, dilation).reshape(seg_shape))
            o_full, lse_full = spread_rows(o_sp, lse_sp, dilation)
            branch_outs.append(o_full)
            branch_lse.append(lse_full)
        lse_max = jnp.max(jnp.stack(branch_lse), axis=0)
        numerator = jnp.zeros_like(branch_outs[0])
        denominator = jnp.zeros_like(lse_max)
        for o_full, lse_full in zip(branch_outs, branch_lse):
            branch_wt = jnp.exp(lse_full - lse_max)
            numerator = numerator + branch_wt[:, :, None] * o_full
            denominator = denominator + branch_wt
        o_mix = (numerator / denominator[:, :, None]).astype(jnp.bfloat16)
        y_seq = jnp.dot(o_mix.reshape(SEQ_LEN, NUM_HEADS * HEAD_DIM), w_o.reshape(NUM_HEADS * HEAD_DIM, MODEL_DIM), preferred_element_type=jnp.float32)
        return y_seq.astype(jnp.bfloat16)

    return lax.map(one_sequence, x)
```

```python
import functools

import jax
import jax.numpy as jnp
from jax import lax
from jax.experimental import pallas as pl
from jax.experimental.pallas import tpu as pltpu
from jax.sharding import PartitionSpec as P


REL = (0, 4, 2, 6, 1, 5, 3, 7)
LOG2E = 1.4426950408889634
F32 = jnp.float32
BF16 = jnp.bfloat16
TILE = 256


def cost(flops, bytes_accessed, transcendentals=0):
    return pl.CostEstimate(flops=int(flops), bytes_accessed=int(bytes_accessed), transcendentals=int(transcendentals))


def onehot(transposed=False):
    dims = (1, 0) if transposed else (0, 1)
    out_row = lax.broadcasted_iota(jnp.int32, (TILE, TILE), dims[0])
    in_row = lax.broadcasted_iota(jnp.int32, (TILE, TILE), dims[1])
    hit = in_row == (out_row % 32) * 8 + out_row // 32
    return jnp.where(hit, 1.0, 0.0).astype(BF16)


def split_kernel(n_sub, a_ref, o_ref):
    take = onehot()
    for sub in range(n_sub):
        rows = jnp.dot(take, a_ref[sub * TILE:(sub + 1) * TILE, :], preferred_element_type=F32).astype(BF16)
        for res in range(8):
            o_ref[res, sub * 32:(sub + 1) * 32, :] = rows[res * 32:(res + 1) * 32]


def split_rows(a, n_sub):
    n_rows, width = a.shape
    blk = n_sub * TILE
    return pl.pallas_call(
        functools.partial(split_kernel, n_sub),
        grid=(n_rows // blk,),
        in_specs=[pl.BlockSpec((blk, width), lambda i: (i, 0))],
        out_specs=pl.BlockSpec((8, blk // 8, width), lambda i: (0, i, 0)),
        out_shape=jax.ShapeDtypeStruct((8, n_rows // 8, width), a.dtype),
        cost_estimate=cost(2 * n_rows * TILE * width, 4 * n_rows * width),
        name="split_rows",
    )(a)


def project_kernel(rels, n_seqs, n_w, whole, x_ref, *refs):
    head = pl.program_id(0)
    w_refs, o_refs = refs[:n_w], refs[n_w:]
    nb = x_ref.shape[1] // n_seqs
    for pos, rel in enumerate(rels):
        rows = x_ref[lax.rem(head + rel, 8)]
        for wi in range(n_w):
            out = jnp.dot(rows, w_refs[wi][0], preferred_element_type=F32).astype(BF16)
            for seq in range(n_seqs):
                part = out[seq * nb:(seq + 1) * nb]
                o_ref, at = (o_refs[0], seq) if whole else (o_refs[seq], 0)
                o_ref[wi, at, 0, pos * nb:(pos + 1) * nb, :] = part
                if whole and len(o_refs) > 1 and pos == 0:
                    o_refs[1][0, seq, 0] = part


def project(xp, ws, rels, n_seqs, whole=True, first_too=False):
    n_w, (_, rows, model_dim), head_dim = len(ws), xp.shape, ws[0].shape[2]
    n_heads, nb, n_pos = ws[0].shape[0], rows // n_seqs, len(rels)
    dims = [(n_w, n_seqs, n_heads, n_pos * nb, head_dim)] if whole else [(n_w, 1, n_heads, n_pos * nb, head_dim)] * n_seqs
    if first_too:
        dims.append((n_w, n_seqs, n_heads, nb, head_dim))
    return pl.pallas_call(
        functools.partial(project_kernel, rels, n_seqs, n_w, whole),
        grid=(n_heads,),
        in_specs=[pl.BlockSpec(xp.shape, lambda h: (0, 0, 0))]
        + [pl.BlockSpec((1, model_dim, head_dim), lambda h: (h, 0, 0)) for _ in ws],
        out_specs=[pl.BlockSpec((d[0], d[1], 1, d[3], d[4]), lambda h: (0, 0, h, 0, 0)) for d in dims],
        out_shape=[jax.ShapeDtypeStruct(d, BF16) for d in dims],
        cost_estimate=cost(2 * n_w * n_heads * n_pos * rows * model_dim * head_dim, 2 * (xp.size + n_w * ws[0].size) + 4 * n_w * n_pos * rows * n_heads * head_dim),
        name="project",
    )(xp, *ws)


def mult_of(group, key_group, level):
    return min(group, key_group) - level + 1


def by_group(groups, values):
    if all(value == 1 for value in values):
        return None
    n_rows = sum(rows for _, rows in groups)
    row = lax.broadcasted_iota(jnp.int32, (n_rows, 1), 0)
    column, base = jnp.full((n_rows, 1), float(values[-1]), F32), n_rows
    for value, (_, rows) in list(zip(values, groups))[::-1]:
        column = jnp.where(row < base, float(value), column)
        base -= rows
    return column


def lane_sum(p):
    total = p[:, :128]
    for lane in range(128, p.shape[1], 128):
        total = total + p[:, lane:lane + 128]
    return total


def scores(q, keys):
    return lax.dot_general(q, keys, (((1,), (1,)), ((), ())), preferred_element_type=F32)


def row_sum(p):
    return jnp.sum(p, axis=1, keepdims=True)


def run_tile(q, k_scr, v_scr, chunks, groups, level, state):
    scale = LOG2E * q.shape[1] ** -0.5
    for start, segs in chunks:
        size = sum(length for length, _ in segs)
        s = scores(q, k_scr[start:start + size, :])
        shift = jnp.max(s, axis=1, keepdims=True) * scale
        if state is not None:
            shift = jnp.maximum(state[0], shift)
        parts, off = [], 0
        for length, key_group in segs:
            mult = by_group(groups, [mult_of(group, key_group, level) for group, _ in groups])
            local = shift if mult is None else shift - jnp.log2(mult)
            parts.append(jnp.exp2(s[:, off:off + length] * scale - local))
            off += length
        p = parts[0] if len(parts) == 1 else jnp.concatenate(parts, axis=1)
        total = row_sum(lane_sum(p))
        acc = jnp.dot(p.astype(BF16), v_scr[start:start + size, :], preferred_element_type=F32)
        if state is not None:
            alpha = jnp.exp2(state[0] - shift)
            total = state[1] * alpha + total
            acc = state[2] * alpha + acc
        state = (shift, total, acc)
    return state


def run_branch0(q, k_scr, v_scr, chunks, groups, s_scr, p_scr):
    scale = LOG2E * q.shape[1] ** -0.5
    peak = None
    for start, segs in chunks:
        size = sum(length for length, _ in segs)
        s = scores(q, k_scr[start:start + size, :])
        s_scr[:, start:start + size] = s
        top = s[:, :128]
        for lane in range(128, size, 128):
            top = jnp.maximum(top, s[:, lane:lane + 128])
        peak = top if peak is None else jnp.maximum(peak, top)
    shift = jnp.max(peak, axis=1, keepdims=True) * scale
    sums = {}
    for start, segs in chunks:
        for length, key_group in segs:
            p = jnp.exp2(s_scr[:, start:start + length] * scale - shift)
            s_scr[:, start:start + length] = p
            part = lane_sum(p)
            sums[key_group] = part if key_group not in sums else sums[key_group] + part
            start += length
    sums = {key_group: row_sum(part) for key_group, part in sums.items()}
    total = functools.reduce(jnp.add, sums.values())
    inverse = 1.0 / total
    factors = {}
    for key_group in sums:
        mult = by_group(groups, [mult_of(group, key_group, 0) for group, _ in groups])
        factors[key_group] = inverse if mult is None else inverse * mult
    for start, segs in chunks:
        for length, key_group in segs:
            p_scr[:, start:start + length] = (s_scr[:, start:start + length] * factors[key_group]).astype(BF16)
            start += length
    acc = jnp.dot(p_scr[...], v_scr[...], preferred_element_type=F32)
    weight = functools.reduce(jnp.add, [sums[key_group] * factors[key_group] for key_group in sums])
    return shift + jnp.log2(total), weight, acc


def merge(one, two):
    shift = jnp.maximum(one[0], two[0])
    w_one, w_two = jnp.exp2(one[0] - shift), jnp.exp2(two[0] - shift)
    return shift, one[1] * w_one + two[1] * w_two, one[2] * w_one + two[2] * w_two


def gather_keys(kv_refs, k_scr, v_scr):
    off = 0
    for ref in kv_refs:
        rows = ref.shape[3]
        k_scr[off:off + rows, :] = ref[0, 0, 0]
        v_scr[off:off + rows, :] = ref[1, 0, 0]
        off += rows


def put_state(acc_ref, stat_ref, state):
    shift, total, acc = state
    lane = lax.broadcasted_iota(jnp.int32, (shift.shape[0], 128), 1)
    acc_ref[0, 0] = acc
    stat_ref[0, 0] = jnp.where(lane < 64, shift, total)


def get_state(acc_ref, stat_ref):
    stat = stat_ref[0, 0]
    return stat[:, 0:1], stat[:, 64:65], acc_ref[0, 0]


def cut(state, lo, hi):
    return tuple(part[lo:hi] for part in state)


def finish(state):
    return (state[2] / state[1]).astype(BF16)


def level0_kernel(nb, q_ref, *refs):
    kv_refs, (o_ref, acc_ref, stat_ref, k_scr, v_scr, s_scr, p_scr) = refs[:8], refs[8:]
    gather_keys(kv_refs, k_scr, v_scr)
    chunks = ((0, ((2 * nb, 3), (2 * nb, 2))), (4 * nb, ((4 * nb, 1),)), (8 * nb, ((4 * nb, 0),)), (12 * nb, ((4 * nb, 0),)))
    low = run_branch0(q_ref[0, 0, 0, :4 * nb, :], k_scr, v_scr, chunks, ((3, nb), (2, nb), (1, 2 * nb)), s_scr, p_scr)
    put_state(acc_ref, stat_ref, low)
    high = run_branch0(q_ref[0, 0, 0, 4 * nb:, :], k_scr, v_scr, chunks, ((0, 4 * nb),), s_scr, p_scr)
    o_ref[0, 0] = finish(high)


def level1_kernel(nb, q_ref, *refs):
    kv_refs, (acc_in, stat_in, acc_two, stat_two, far_ref, o_ref, k_scr, v_scr) = refs[:6], refs[6:]
    gather_keys(kv_refs, k_scr, v_scr)
    chunks = ((0, ((2 * nb, 3), (2 * nb, 2))), (4 * nb, ((4 * nb, 1),)))
    state = run_tile(q_ref[0, 0, 0], k_scr, v_scr, chunks, ((3, nb), (2, nb), (1, 2 * nb)), 1, get_state(acc_in, stat_in))
    o_ref[0, 0, 2 * nb:, :] = finish(cut(state, 2 * nb, 4 * nb))
    two = get_state(acc_two, stat_two)
    o_ref[0, 0, nb:2 * nb, :] = finish(merge(cut(state, nb, 2 * nb), cut(two, nb, 2 * nb)))

    def column(lane):
        return jnp.transpose(jnp.broadcast_to(far_ref[0, 0, nb:nb + 1, lane:lane + nb], (128, nb)))[:, 0:1]

    far = (column(0), column(128), far_ref[0, 0, :nb, :])
    o_ref[0, 0, :nb, :] = finish(merge(merge(cut(state, 0, nb), cut(two, 0, nb)), far))


def level2_kernel(nb, q_ref, *refs):
    kv_refs, (acc_ref, stat_ref, k_scr, v_scr) = refs[:8], refs[8:]
    gather_keys(kv_refs, k_scr, v_scr)
    chunks = ((0, ((4 * nb, 3),)), (4 * nb, ((4 * nb, 2),)))
    put_state(acc_ref, stat_ref, run_tile(q_ref[0, 0, 0], k_scr, v_scr, chunks, ((3, nb), (2, nb)), 2, None))


def level3_kernel(nb, q_ref, *refs):
    kv_refs, (far_ref, k_scr, v_scr) = refs[:8], refs[8:]
    gather_keys(kv_refs, k_scr, v_scr)
    shift, total, acc = run_tile(q_ref[0, 0, 0], k_scr, v_scr, ((0, ((8 * nb, 3),)),), ((3, nb),), 3, None)
    far_ref[0, 0, :nb, :] = acc
    far_ref[0, 0, nb:, 0:nb] = jnp.transpose(jnp.broadcast_to(shift, (nb, 128)))[0:8, :]
    far_ref[0, 0, nb:, 128:128 + nb] = jnp.transpose(jnp.broadcast_to(total, (nb, 128)))[0:8, :]


def attend(body, nb, q, q_rows, kvs, states, outs, seqs, with_scores=False):
    n_heads, head_dim = q.shape[2], q.shape[4]
    n_keys = sum(kv.shape[3] for kv in kvs)
    first, n_seqs = seqs

    def spec(n_here, rows, width):
        base = first if n_here > n_seqs else 0
        return pl.BlockSpec((1, 1, rows, width), lambda s, h: (s + base, h, 0, 0))

    def lead_spec(lead, n_here, rows):
        base = first if n_here > n_seqs else 0
        return pl.BlockSpec((lead, 1, 1, rows, head_dim), lambda s, h: (0, s + base, h, 0, 0))

    pairs = n_seqs * n_heads * q_rows * n_keys
    scratch = [pltpu.VMEM((n_keys, head_dim), BF16)] * 2
    if with_scores:
        scratch += [pltpu.VMEM((q_rows // 2, n_keys), F32), pltpu.VMEM((q_rows // 2, n_keys), BF16)]
    return pl.pallas_call(
        functools.partial(body, nb),
        grid=(n_seqs, n_heads),
        in_specs=[lead_spec(1, q.shape[1], q_rows)]
        + [lead_spec(2, kv.shape[1], kv.shape[3]) for kv in kvs]
        + [spec(state.shape[0], *state.shape[2:]) for state in states],
        out_specs=[spec(n_seqs, rows, width) for rows, width, _ in outs],
        out_shape=[jax.ShapeDtypeStruct((n_seqs, n_heads, rows, width), dtype) for rows, width, dtype in outs],
        scratch_shapes=scratch,
        cost_estimate=cost(4 * pairs * head_dim, 2 * n_seqs * n_heads * head_dim * (q_rows + 2 * n_keys), pairs),
    )(q, *kvs, *states)


def out_kernel(nb, n_sub, o_low, o_high, w_ref, *refs):
    y_ref, mix, lhs = refs[-3:]
    blk = pl.program_id(0)
    back = onehot(transposed=True)
    for sub in range(n_sub):
        first = pl.multiple_of((blk * n_sub + sub) * 32, 32)
        for res in range(8):
            for head in range(8):
                pos = REL[(res - head) % 8]
                ref, base = (o_low, 0) if pos < 4 else (o_high, 4)
                piece = ref[0, head, pl.ds((pos - base) * nb + first, 32), :]
                mix[res * 32:(res + 1) * 32, head * piece.shape[1]:(head + 1) * piece.shape[1]] = piece
        lhs[sub * TILE:(sub + 1) * TILE, :] = jnp.dot(back, mix[...], preferred_element_type=F32).astype(BF16)
    y_ref[0] = jnp.dot(lhs[...], w_ref[...], preferred_element_type=F32).astype(BF16)


def out_project(o_low, o_high, w, nb, seq, n_seqs, y_prev):
    width, model_dim = w.shape
    n_tok = nb * 8
    n_sub = min(2, n_tok // TILE)
    blk = n_sub * TILE
    in_specs = [pl.BlockSpec(a.shape, lambda i: (0, 0, 0, 0)) for a in (o_low, o_high)] + [pl.BlockSpec(w.shape, lambda i: (0, 0))]
    more = () if y_prev is None else (y_prev,)
    return pl.pallas_call(
        functools.partial(out_kernel, nb, n_sub),
        grid=(n_tok // blk,),
        in_specs=in_specs + [pl.BlockSpec(memory_space=pl.ANY) for _ in more],
        out_specs=pl.BlockSpec((1, blk, model_dim), lambda i: (seq, i, 0)),
        out_shape=jax.ShapeDtypeStruct((n_seqs, n_tok, model_dim), BF16),
        scratch_shapes=[pltpu.VMEM((TILE, width), BF16), pltpu.VMEM((blk, width), BF16)],
        input_output_aliases={3: 0} if more else {},
        cost_estimate=cost(2 * n_tok * width * model_dim, 4 * n_tok * width + 2 * w.size),
        name="out_project",
    )(o_low, o_high, w, *more)


def solution(mesh):
    n_dev = mesh.shape['sp']

    def swap(a, bit):
        return lax.ppermute(a, 'sp', [(d, d ^ bit) for d in range(n_dev)])

    def local_step(x_loc, w_q, w_k, w_v, w_o):
        n_seqs, n_tok, model_dim = x_loc.shape
        n_heads, head_dim = w_q.shape[1], w_q.shape[2]
        nb = n_tok // 8
        n_rows = n_seqs * n_tok
        after = lax.optimization_barrier

        def per_head(w):
            rows = w.reshape(model_dim * n_heads, head_dim)
            return split_rows(rows, 8 if rows.shape[0] % (8 * TILE) == 0 else 1)

        xp = split_rows(x_loc.reshape(n_rows, model_dim), 2 if n_rows % 512 == 0 else 1)
        wk, wv = per_head(w_k), per_head(w_v)

        e, = project(xp, (wk, wv), REL[0:1], n_seqs)
        wk, wv, e = after((wk, wv, e))
        y_e, z_e, c_e = swap(e, 2), swap(e, 4), swap(e, 1)
        b, = project(xp, (wk, wv), REL[1:2], n_seqs)
        wk, wv, b = after((wk, wv, b))
        y_b, z_b, c_b = swap(b, 2), swap(b, 4), swap(b, 1)
        g = project(xp, (wk, wv), REL[2:4], n_seqs, whole=False)
        wk, wv, g = after((wk, wv, g))
        y_g = [swap(g[0], 2)]
        c_g = [swap(g[0], 1), swap(g[1], 1)]
        r, = project(xp, (wk, wv), REL[4:8], n_seqs)
        w_q, r = after((w_q, r))
        c_r = swap(r, 1)
        wq = per_head(w_q)
        q_all, q_first = project(xp, (wq,), REL, n_seqs, first_too=True)

        q_all, q_first, y_e, z_e = after((q_all, q_first, y_e, z_e))
        zy_e, yc_e, zc_e = swap(y_e, 4), swap(y_e, 1), swap(z_e, 1)
        q_far = swap(q_first, 8)

        def level0(seq, q):
            kvs = (e, c_e, b, c_b, g[seq], c_g[seq], r, c_r)
            return attend(level0_kernel, nb, q, 8 * nb, kvs, (),
                          ((4 * nb, head_dim, BF16), (4 * nb, head_dim, F32), (4 * nb, 128, F32)), (seq, 1), with_scores=True)

        near0 = level0(0, q_all)
        near0, q_all, y_b, z_b, g1 = after((near0, q_all, y_b, z_b, g[1]))
        zy_b, yc_b, zc_b = swap(z_b, 2), swap(y_b, 1), swap(z_b, 1)
        y_g.append(swap(g1, 2))
        near1 = level0(1, q_all)
        near1, q_all, q_far, zy_e, y_g[0] = after((near1, q_all, q_far, zy_e, y_g[0]))
        near = (near0, near1)
        zyc_e = swap(zy_e, 1)
        yc_g = [swap(y_g[0], 1)]
        far, = attend(level3_kernel, nb, q_far, nb, (e, c_e, y_e, yc_e, z_e, zc_e, zy_e, zyc_e), (),
                      ((nb + 8, head_dim, F32),), (0, n_seqs))
        far_in = swap(far, 8)
        far, q_all, zy_b = after((far, q_all, zy_b))
        zyc_b = swap(zy_b, 1)
        two = attend(level2_kernel, nb, q_all, 2 * nb, (z_e, zc_e, zy_e, zyc_e, z_b, zc_b, zy_b, zyc_b), (),
                     ((2 * nb, head_dim, F32), (2 * nb, 128, F32)), (0, n_seqs))
        y = None
        w_out = w_o.reshape(n_heads * head_dim, model_dim)
        for seq in range(n_seqs):
            o_high, acc, stat = near[seq]
            kvs = (y_e, yc_e, y_b, yc_b, y_g[seq], yc_g[seq])
            o_low, = attend(level1_kernel, nb, q_all, 4 * nb, kvs, (acc, stat, *two, far_in), ((4 * nb, head_dim, BF16),), (seq, 1))
            if seq == 0:
                o_low, y_g[1] = after((o_low, y_g[1]))
                yc_g.append(swap(y_g[1], 1))
            y = out_project(o_low, o_high, w_out, nb, seq, n_seqs, y)
        return y

    return jax.shard_map(local_step, mesh=mesh, in_specs=(P('dp', 'sp', None), P(), P(), P(), P()), out_specs=P('dp', 'sp', None), check_vma=False)
```

```python
import functools

import jax
import jax.numpy as jnp
from jax import lax
from jax.experimental import pallas as pl
from jax.experimental.pallas import tpu as pltpu
from jax.sharding import PartitionSpec as P


SLOT = (0, 4, 2, 6, 1, 5, 3, 7)
LOG2E = 1.4426950408889634
F32 = jnp.float32
BF16 = jnp.bfloat16
TILE = 256


def cost(flops, bytes_accessed, transcendentals=0):
    return pl.CostEstimate(flops=int(flops), bytes_accessed=int(bytes_accessed), transcendentals=int(transcendentals))


def swap_bits(head):
    return (head % 2) * 4 + (head // 2 % 2) * 2 + head // 4


def position(slot, own):
    if slot == own:
        return 0
    if slot // 2 == own // 2:
        return 1
    return 2 + slot % 2 if slot // 4 == own // 4 else 4 + slot % 4


def onehot(transposed=False):
    dims = (1, 0) if transposed else (0, 1)
    out_row = lax.broadcasted_iota(jnp.int32, (TILE, TILE), dims[0])
    in_row = lax.broadcasted_iota(jnp.int32, (TILE, TILE), dims[1])
    hit = in_row == (out_row % 32) * 8 + out_row // 32
    return jnp.where(hit, 1.0, 0.0).astype(BF16)


def split_kernel(n_sub, slots, *refs):
    take = onehot()
    half = len(refs) // 2
    for sub in range(n_sub):
        for a_ref, o_ref in zip(refs[:half], refs[half:]):
            rows = jnp.dot(take, a_ref[sub * TILE:(sub + 1) * TILE, :], preferred_element_type=F32).astype(BF16)
            for res in range(8):
                o_ref[slots[res], sub * 32:(sub + 1) * 32, :] = rows[res * 32:(res + 1) * 32]


def split_rows(arrays, n_sub, slots=tuple(range(8))):
    n_rows, width = arrays[0].shape
    blk = n_sub * TILE
    return pl.pallas_call(
        functools.partial(split_kernel, n_sub, slots),
        grid=(n_rows // blk,),
        in_specs=[pl.BlockSpec((blk, width), lambda i: (i, 0)) for _ in arrays],
        out_specs=[pl.BlockSpec((8, blk // 8, width), lambda i: (0, i, 0)) for _ in arrays],
        out_shape=[jax.ShapeDtypeStruct((8, n_rows // 8, width), BF16) for _ in arrays],
        cost_estimate=cost(2 * len(arrays) * n_rows * TILE * width, 4 * len(arrays) * n_rows * width),
        name="split_rows",
    )(*arrays)


def near_kernel(n_seqs, x_ref, *refs):
    w_refs, (e_ref, b_ref) = refs[:2], refs[2:]
    nb = x_ref.shape[0] // (2 * n_seqs)
    own = pl.program_id(0)
    for wi, w_ref in enumerate(w_refs):
        out = jnp.dot(x_ref[...], w_ref[0], preferred_element_type=F32).astype(BF16)
        for parity in range(2):
            @pl.when(own % 2 == parity)
            def _():
                for slot, o_ref in ((parity, e_ref), (1 - parity, b_ref)):
                    for seq in range(n_seqs):
                        at = (slot * n_seqs + seq) * nb
                        o_ref[wi, seq, 0] = out[at:at + nb]


def rest_kernel(n_seqs, x_ref, *refs):
    w_refs, g_refs, r_ref = refs[:2], refs[2:2 + n_seqs], refs[2 + n_seqs]
    rows = x_ref.shape[0] // 8
    nb = rows // n_seqs
    own = pl.program_id(0)
    pair = pl.ds(pl.multiple_of((own // 2 + 1 - 2 * (own // 2 % 2)) * 2 * rows, 2 * rows), 2 * rows)
    half = pl.ds(pl.multiple_of((1 - own // 4) * 4 * rows, 4 * rows), 4 * rows)
    for wi, w_ref in enumerate(w_refs):
        out = jnp.dot(x_ref[pair, :], w_ref[0], preferred_element_type=F32).astype(BF16)
        for slot in range(2):
            for seq in range(n_seqs):
                at = (slot * n_seqs + seq) * nb
                g_refs[seq][wi, 0, 0, slot * nb:(slot + 1) * nb, :] = out[at:at + nb]
        out = jnp.dot(x_ref[half, :], w_ref[0], preferred_element_type=F32).astype(BF16)
        for slot in range(4):
            for seq in range(n_seqs):
                at = (slot * n_seqs + seq) * nb
                r_ref[wi, seq, 0, slot * nb:(slot + 1) * nb, :] = out[at:at + nb]


def query_kernel(n_seqs, x_ref, w_ref, q_ref, *first_refs):
    rows = x_ref.shape[0] // 8
    nb = rows // n_seqs
    own = pl.program_id(0)
    out = jnp.dot(x_ref[...], w_ref[0], preferred_element_type=F32).astype(BF16)
    for slot in range(8):
        same_half = 1 - jnp.abs(slot // 4 - own // 4)
        same_pair = jnp.where(slot // 2 == own // 2, 1, 0)
        same = jnp.where(slot == own, 1, 0)
        pos = jnp.where(same == 1, 0, jnp.where(same_pair == 1, 1, jnp.where(same_half == 1, 2 + slot % 2, 4 + slot % 4)))
        for seq in range(n_seqs):
            at = (slot * n_seqs + seq) * nb
            q_ref[0, seq, 0, pl.ds(pl.multiple_of(pos * nb, nb), nb), :] = out[at:at + nb]
    for seq in range(n_seqs):
        first_refs[seq][0, 0, 0] = q_ref[0, seq, 0, :nb, :]


def project(kernel, xp, ws, n_seqs, outs, x_pair=False):
    n_heads, model_dim, head_dim = ws[0].shape
    rows = xp.shape[0]
    x_rows = rows // 4 if x_pair else rows
    out_rows = sum(n_w * seqs * n for n_w, seqs, n in outs)
    return pl.pallas_call(
        functools.partial(kernel, n_seqs),
        grid=(n_heads,),
        in_specs=[pl.BlockSpec((x_rows, model_dim), (lambda g: (g // 2, 0)) if x_pair else (lambda g: (0, 0)))]
        + [pl.BlockSpec((1, model_dim, head_dim), lambda g: (swap_bits(g), 0, 0)) for _ in ws],
        out_specs=[pl.BlockSpec((n_w, seqs, 1, n, head_dim), lambda g: (0, 0, swap_bits(g), 0, 0)) for n_w, seqs, n in outs],
        out_shape=[jax.ShapeDtypeStruct((n_w, seqs, n_heads, n, head_dim), BF16) for n_w, seqs, n in outs],
        cost_estimate=cost(2 * n_heads * out_rows * model_dim * head_dim, 2 * (xp.size + len(ws) * ws[0].size) + 2 * n_heads * out_rows * head_dim),
        name="project",
    )(xp, *ws)


def mult_of(group, key_group, level):
    return min(group, key_group) - level + 1


LOG2 = {1: 0.0, 2: 1.0, 3: 1.584962500721156, 4: 2.0}


def by_group(groups, key_group, level, log=False):
    mults = [mult_of(group, key_group, level) for group, _ in groups]
    if all(mult == 1 for mult in mults):
        return None
    values = [LOG2[mult] if log else float(mult) for mult in mults]
    n_cols = sum(cols for _, cols in groups)
    col = lax.broadcasted_iota(jnp.int32, (1, n_cols), 1)
    row, base = jnp.full((1, n_cols), values[-1], F32), n_cols
    for value, (_, cols) in list(zip(values, groups))[::-1]:
        row = jnp.where(col < base, value, row)
        base -= cols
    return row


def scores(keys, q):
    return lax.dot_general(keys, q, (((1,), (1,)), ((), ())), preferred_element_type=F32)


def fold(op, p):
    return op(p.reshape(p.shape[0] // 8, 8, p.shape[1]), axis=0)


def gather_keys(kv_refs, k_scr, v_scr):
    off = 0
    for ref in kv_refs:
        rows = ref.shape[3]
        k_scr[off:off + rows, :] = ref[0, 0, 0]
        v_scr[:, off:off + rows] = jnp.transpose(ref[1, 0, 0])
        off += rows


def run_branch0(q, k_scr, v_scr, segs, step, groups, s_scr, p_scr):
    scale = LOG2E * q.shape[1] ** -0.5
    peak = None
    for start in range(0, k_scr.shape[0], step):
        s = scores(k_scr[start:start + step, :], q)
        s_scr[start:start + step, :] = s
        top = fold(jnp.max, s)
        peak = top if peak is None else jnp.maximum(peak, top)
    shift = jnp.max(peak, axis=0, keepdims=True) * scale
    sums, start = [], 0
    for length, _ in segs:
        p = jnp.exp2(s_scr[start:start + length, :] * scale - shift)
        s_scr[start:start + length, :] = p
        sums.append(jnp.sum(fold(jnp.sum, p), axis=0, keepdims=True))
        start += length
    total = functools.reduce(jnp.add, sums)
    inverse = 1.0 / total
    weight, start = None, 0
    for (length, key_group), part in zip(segs, sums):
        mult = by_group(groups, key_group, 0)
        factor = inverse if mult is None else inverse * mult
        p_scr[start:start + length, :] = (s_scr[start:start + length, :] * factor).astype(BF16)
        weight = part * factor if weight is None else weight + part * factor
        start += length
    acc = jnp.dot(v_scr[...], p_scr[...], preferred_element_type=F32)
    return shift + jnp.log2(total), weight, acc


def level0_kernel(nb, q_ref, *refs):
    kv_refs, (o_ref, acc_ref, stat_ref, k_scr, v_scr, s_scr, p_scr, s_scr2, p_scr2) = refs[:8], refs[8:]
    gather_keys(kv_refs, k_scr, v_scr)
    segs = ((2 * nb, 3), (2 * nb, 2), (4 * nb, 1), (8 * nb, 0))
    groups = ((3, nb), (2, nb), (1, 2 * nb))
    shift, weight, acc = run_branch0(q_ref[0, 0, 0, :4 * nb, :], k_scr, v_scr, segs, 4 * nb, groups, s_scr, p_scr)
    acc_ref[0, 0] = acc
    stat_ref[0, 0, 0:1, :] = shift
    stat_ref[0, 0, 1:2, :] = weight
    _, _, acc = run_branch0(q_ref[0, 0, 0, 4 * nb:, :], k_scr, v_scr, segs, 4 * nb, ((0, 4 * nb),), s_scr2, p_scr2)
    o_ref[0, 0] = jnp.transpose(acc).astype(BF16)


def weights(s, shift, scale, segs, groups, level, p_scr):
    start, total = 0, None
    for length, key_group in segs:
        mult = by_group(groups, key_group, level, log=True)
        local = shift if mult is None else shift - mult
        p = jnp.exp2(s[start:start + length, :] * scale - local)
        p_scr[start:start + length, :] = p.astype(BF16)
        part = fold(jnp.sum, p)
        total = part if total is None else total + part
        start += length
    return jnp.sum(total, axis=0, keepdims=True)


def peak_of(s, scale):
    return jnp.max(fold(jnp.max, s), axis=0, keepdims=True) * scale


def upper(op, low, row):
    n_cols = low.shape[1]
    return jnp.concatenate([op(row[:, :n_cols], low), row[:, n_cols:]], axis=1)


def final_kernel(nb, q_ref, *refs):
    one_refs, two_refs, refs = refs[:6], refs[6:14], refs[14:]
    acc_in, stat_in, far_ref, o_ref, k_one, v_one, k_two, v_two, p_one, p_two = refs
    gather_keys(one_refs, k_one, v_one)
    gather_keys(two_refs, k_two, v_two)
    head_dim = q_ref.shape[4]
    scale = LOG2E * head_dim ** -0.5
    s_one = scores(k_one[...], q_ref[0, 0, 0])
    s_two = scores(k_two[...], q_ref[0, 0, 0, :2 * nb, :])
    shift_near, sum_near = stat_in[0, 0, 0:1, :], stat_in[0, 0, 1:2, :]
    shift_far, sum_far = far_ref[0, 0, head_dim:head_dim + 1, :], far_ref[0, 0, head_dim + 1:head_dim + 2, :]
    shift = jnp.maximum(shift_near, peak_of(s_one, scale))
    shift = upper(jnp.maximum, peak_of(s_two, scale), shift)
    shift = upper(jnp.maximum, shift_far, shift)
    low, mid, high = (3, nb), (2, nb), (1, 2 * nb)
    sum_one = weights(s_one, shift, scale, ((2 * nb, 3), (2 * nb, 2), (4 * nb, 1)), (low, mid, high), 1, p_one)
    sum_two = weights(s_two, shift[:, :2 * nb], scale, ((4 * nb, 3), (4 * nb, 2)), (low, mid), 2, p_two)
    near_scale = jnp.exp2(shift_near - shift)
    far_scale = jnp.exp2(shift_far - shift[:, :nb])
    total = upper(jnp.add, sum_far * far_scale, upper(jnp.add, sum_two, sum_near * near_scale + sum_one))
    inverse = 1.0 / total
    acc = acc_in[0, 0] * near_scale + jnp.dot(v_one[...], p_one[...], preferred_element_type=F32)
    acc_two = jnp.dot(v_two[...], p_two[...], preferred_element_type=F32)
    acc_two = upper(jnp.add, far_ref[0, 0, :head_dim, :] * far_scale, acc_two)
    acc = upper(jnp.add, acc_two, acc)
    o_ref[0, 0] = jnp.transpose(acc * inverse).astype(BF16)


def far_kernel(nb, q_ref, *refs):
    kv_refs, (far_ref, k_scr, v_scr, p_scr) = refs[:8], refs[8:]
    gather_keys(kv_refs, k_scr, v_scr)
    head_dim = q_ref.shape[4]
    scale = LOG2E * head_dim ** -0.5
    s = scores(k_scr[...], q_ref[0, 0, 0])
    shift = peak_of(s, scale)
    total = weights(s, shift, scale, ((8 * nb, 3),), ((3, nb),), 3, p_scr)
    far_ref[0, 0, :head_dim, :] = jnp.dot(v_scr[...], p_scr[...], preferred_element_type=F32)
    far_ref[0, 0, head_dim:, :] = jnp.concatenate([shift, total] + [jnp.zeros_like(shift)] * 6, axis=0)


def attend(body, nb, q, q_rows, kvs, states, outs, seq, scratch, pairs):
    n_heads, head_dim = q.shape[2], q.shape[4]
    n_keys = sum(kv.shape[3] for kv in kvs)

    def spec(n_here, *dims):
        base = seq if n_here > 1 else 0
        return pl.BlockSpec((1, 1, *dims), lambda h: (base, h, 0, 0))

    def lead_spec(lead, n_here, rows):
        base = seq if n_here > 1 else 0
        return pl.BlockSpec((lead, 1, 1, rows, head_dim), lambda h: (0, base, h, 0, 0))

    return pl.pallas_call(
        functools.partial(body, nb),
        grid=(n_heads,),
        in_specs=[lead_spec(1, q.shape[1], q_rows)]
        + [lead_spec(2, kv.shape[1], kv.shape[3]) for kv in kvs]
        + [spec(state.shape[0], *state.shape[2:]) for state in states],
        out_specs=[spec(1, rows, width) for rows, width, _ in outs],
        out_shape=[jax.ShapeDtypeStruct((1, n_heads, rows, width), dtype) for rows, width, dtype in outs],
        scratch_shapes=[pltpu.VMEM(dims, dtype) for dims, dtype in scratch],
        cost_estimate=cost(4 * n_heads * pairs * head_dim, 2 * n_heads * head_dim * (q_rows + 2 * n_keys), n_heads * pairs),
    )(q, *kvs, *states)


def out_kernel(nb, o_low, o_high, w_ref, *refs):
    y_ref, mix, lhs = refs[-3:]
    n_tok = lhs.shape[0]

    @pl.when(pl.program_id(0) == 0)
    def _():
        back = onehot(transposed=True)
        for sub in range(n_tok // TILE):
            for res in range(8):
                for head in range(8):
                    pos = position(SLOT[res], SLOT[head])
                    ref, base = (o_low, 0) if pos < 4 else (o_high, 4)
                    first = (pos - base) * nb + sub * 32
                    piece = ref[0, head, first:first + 32, :]
                    mix[res * 32:(res + 1) * 32, head * piece.shape[1]:(head + 1) * piece.shape[1]] = piece
            lhs[sub * TILE:(sub + 1) * TILE, :] = jnp.dot(back, mix[...], preferred_element_type=F32).astype(BF16)

    y_ref[0] = jnp.dot(lhs[...], w_ref[...], preferred_element_type=F32).astype(BF16)


def out_project(o_low, o_high, w, nb, seq, n_seqs, y_prev):
    width, model_dim = w.shape
    n_tok = nb * 8
    n_cols = min(512, model_dim)
    in_specs = [pl.BlockSpec(a.shape, lambda i: (0, 0, 0, 0)) for a in (o_low, o_high)] + [pl.BlockSpec((width, n_cols), lambda i: (0, i))]
    more = () if y_prev is None else (y_prev,)
    return pl.pallas_call(
        functools.partial(out_kernel, nb),
        grid=(model_dim // n_cols,),
        in_specs=in_specs + [pl.BlockSpec(memory_space=pl.ANY) for _ in more],
        out_specs=pl.BlockSpec((1, n_tok, n_cols), lambda i: (seq, 0, i)),
        out_shape=jax.ShapeDtypeStruct((n_seqs, n_tok, model_dim), BF16),
        scratch_shapes=[pltpu.VMEM((TILE, width), BF16), pltpu.VMEM((n_tok, width), BF16)],
        input_output_aliases={3: 0} if more else {},
        cost_estimate=cost(2 * n_tok * width * model_dim, 4 * n_tok * width + 2 * w.size),
        name="out_project",
    )(o_low, o_high, w, *more)


def solution(mesh):
    n_dev = mesh.shape['sp']

    def swap(a, bit):
        return lax.ppermute(a, 'sp', [(d, d ^ bit) for d in range(n_dev)])

    def local_step(x_loc, w_q, w_k, w_v, w_o):
        n_seqs, n_tok, model_dim = x_loc.shape
        n_heads, head_dim = w_q.shape[1], w_q.shape[2]
        nb = n_tok // 8
        n_rows = n_seqs * n_tok
        after = lax.optimization_barrier

        def per_head(*ws):
            rows = [w.reshape(model_dim * n_heads, head_dim) for w in ws]
            return split_rows(rows, 8 if rows[0].shape[0] % (8 * TILE) == 0 else 1)

        xp, = split_rows((x_loc.reshape(n_rows, model_dim),), 1, SLOT)
        xp = xp.reshape(n_rows, model_dim)
        wk, wv = per_head(w_k, w_v)

        e, b = project(near_kernel, xp, (wk, wv), n_seqs, ((2, n_seqs, nb), (2, n_seqs, nb)), x_pair=True)
        wk, wv, e, b = after((wk, wv, e, b))
        y_e, z_e, c_e = swap(e, 2), swap(e, 4), swap(e, 1)
        y_b, z_b, c_b = swap(b, 2), swap(b, 4), swap(b, 1)
        *g, r = project(rest_kernel, xp, (wk, wv), n_seqs, ((2, 1, 2 * nb),) * n_seqs + ((2, n_seqs, 4 * nb),))
        w_q, g, r = after((w_q, g, r))
        y_g = [swap(g[0], 2)]
        c_g = [swap(g[0], 1), swap(g[1], 1)]
        c_r = swap(r, 1)
        wq, = per_head(w_q)
        q_all, *q_first = project(query_kernel, xp, (wq,), n_seqs, ((1, n_seqs, 8 * nb),) + ((1, 1, nb),) * n_seqs)

        q_all, q_first, y_e, z_e = after((q_all, q_first, y_e, z_e))
        zy_e, yc_e, zc_e = swap(y_e, 4), swap(y_e, 1), swap(z_e, 1)
        q_far = [swap(q_first[seq], 8) for seq in range(n_seqs)]

        def level0(seq, q):
            kvs = (e, c_e, b, c_b, g[seq], c_g[seq], r, c_r)
            keys = 16 * nb
            scratch = [((keys, head_dim), BF16), ((head_dim, keys), BF16)] + [((keys, 4 * nb), F32), ((keys, 4 * nb), BF16)] * 2
            return attend(level0_kernel, nb, q, 8 * nb, kvs, (),
                          ((4 * nb, head_dim, BF16), (head_dim, 4 * nb, F32), (8, 4 * nb, F32)), seq, scratch, 8 * nb * keys)

        near0 = level0(0, q_all)
        near0, q_all, y_b, z_b, g1 = after((near0, q_all, y_b, z_b, g[1]))
        zy_b, yc_b, zc_b = swap(z_b, 2), swap(y_b, 1), swap(z_b, 1)
        y_g.append(swap(g1, 2))
        near1 = level0(1, q_all)
        near1, q_all, q_far, zy_e, y_g[0] = after((near1, q_all, q_far, zy_e, y_g[0]))
        near = (near0, near1)
        zyc_e = swap(zy_e, 1)
        yc_g = [swap(y_g[0], 1)]
        far_in = []
        for seq in range(n_seqs):
            kvs = (e, c_e, y_e, yc_e, z_e, zc_e, zy_e, zyc_e)
            scratch = [((8 * nb, head_dim), BF16), ((head_dim, 8 * nb), BF16), ((8 * nb, nb), BF16)]
            far, = attend(far_kernel, nb, q_far[seq], nb, kvs, (), ((head_dim + 8, nb, F32),), seq, scratch, 8 * nb * nb)
            far_in.append(swap(far, 8))
        far, q_all, zy_b = after((far, q_all, zy_b))
        zyc_b = swap(zy_b, 1)
        y = None
        w_out = w_o.reshape(n_heads * head_dim, model_dim)
        for seq in range(n_seqs):
            o_high, acc, stat = near[seq]
            kvs = (y_e, yc_e, y_b, yc_b, y_g[seq], yc_g[seq], z_e, zc_e, zy_e, zyc_e, z_b, zc_b, zy_b, zyc_b)
            scratch = [((8 * nb, head_dim), BF16), ((head_dim, 8 * nb), BF16)] * 2 + [((8 * nb, 4 * nb), BF16), ((8 * nb, 2 * nb), BF16)]
            o_low, = attend(final_kernel, nb, q_all, 4 * nb, kvs, (acc, stat, far_in[seq]), ((4 * nb, head_dim, BF16),), seq,
                            scratch, 8 * nb * 6 * nb)
            if seq == 0:
                o_low, y_g[1] = after((o_low, y_g[1]))
                yc_g.append(swap(y_g[1], 1))
            y = out_project(o_low, o_high, w_out, nb, seq, n_seqs, y)
        return y

    return jax.shard_map(local_step, mesh=mesh, in_specs=(P('dp', 'sp', None), P(), P(), P(), P()), out_specs=P('dp', 'sp', None), check_vma=False)
```

```python
import functools
import math

import jax
import jax.numpy as jnp
from jax import lax
from jax.experimental import pallas as pl
from jax.experimental.pallas import tpu as pltpu
from jax.sharding import PartitionSpec as P


SLOT = (0, 4, 2, 6, 1, 5, 3, 7)
LOG2E = 1.4426950408889634
F32 = jnp.float32
BF16 = jnp.bfloat16
TILE = 256
PARTS = 2


def cost(flops, bytes_accessed, transcendentals=0):
    return pl.CostEstimate(flops=int(flops), bytes_accessed=int(bytes_accessed), transcendentals=int(transcendentals))


def swap_bits(head):
    return (head % 2) * 4 + (head // 2 % 2) * 2 + head // 4


def position(slot, own):
    if slot // 2 == own // 2:
        return int(slot != own)
    return 2 + slot % 2 if slot // 4 == own // 4 else 4 + slot % 4


def onehot(transposed=False):
    dims = (1, 0) if transposed else (0, 1)
    out_row = lax.broadcasted_iota(jnp.int32, (TILE, TILE), dims[0])
    in_row = lax.broadcasted_iota(jnp.int32, (TILE, TILE), dims[1])
    hit = in_row == (out_row % 32) * 8 + out_row // 32
    return jnp.where(hit, 1.0, 0.0).astype(BF16)


def split_block(take, a_refs, o_ref, slots):
    at = 0
    for a_ref in a_refs:
        for start in range(0, a_ref.shape[0], TILE):
            rows = jnp.dot(take, a_ref[start:start + TILE, :], preferred_element_type=F32).astype(BF16)
            for res in range(8):
                o_ref[slots[res], at:at + 32, :] = rows[res * 32:(res + 1) * 32]
            at += 32


def split_kernel(slots, *refs):
    take = onehot()
    n = len(slots)
    parts = len(refs) // n - 1
    for i in range(n):
        split_block(take, refs[i * parts:(i + 1) * parts], refs[n * parts + i], slots[i])


def part_spec(block, parts, part):
    return pl.BlockSpec(block, lambda i: (i * parts + part, 0))


def split_rows(arrays, slots, steps):
    parts = PARTS if all(a.shape[0] // steps % (PARTS * TILE) == 0 for a in arrays) else 1
    return pl.pallas_call(
        functools.partial(split_kernel, slots),
        grid=(steps,),
        in_specs=[part_spec((a.shape[0] // (steps * parts), a.shape[1]), parts, part) for a in arrays for part in range(parts)],
        out_specs=[pl.BlockSpec((8, a.shape[0] // (8 * steps), a.shape[1]), lambda i: (0, i, 0)) for a in arrays],
        out_shape=[jax.ShapeDtypeStruct((8, a.shape[0] // 8, a.shape[1]), BF16) for a in arrays],
        cost_estimate=cost(sum(2 * a.size * TILE for a in arrays), sum(4 * a.size for a in arrays)),
        name="split_rows",
    )(*[a for a in arrays for _ in range(parts)])


def slot_copy(x_hbm, x_scr, sems, slot):
    rows = x_scr.shape[0] // 8
    part = pl.ds(slot * rows if isinstance(slot, int) else pl.multiple_of(slot * rows, rows), rows)
    return pltpu.make_async_copy(x_hbm.at[part, :], x_scr.at[part, :], sems.at[slot])


def joined(w_refs, wi):
    return jnp.concatenate([ref[0] for ref in w_refs[wi * PARTS:(wi + 1) * PARTS]], axis=0)


def near_kernel(n_seqs, x_hbm, *refs):
    w_refs, refs = refs[:2 * PARTS], refs[2 * PARTS:]
    e_ref, b_refs, (x_scr, sems) = refs[0], refs[1:1 + n_seqs], refs[1 + n_seqs:]
    rows = x_scr.shape[0] // 8
    nb = rows // n_seqs
    own = pl.program_id(0)

    @pl.when(own == 0)
    def _():
        for slot in range(8):
            slot_copy(x_hbm, x_scr, sems, slot).start()

    @pl.when(own % 2 == 0)
    def _():
        slot_copy(x_hbm, x_scr, sems, own).wait()
        slot_copy(x_hbm, x_scr, sems, own + 1).wait()

    mine = x_scr[pl.ds(pl.multiple_of(own * rows, rows), rows), :]
    other = x_scr[pl.ds(pl.multiple_of((own + 1 - 2 * (own % 2)) * rows, rows), rows), :]
    both = jnp.concatenate([mine, other], axis=0)
    for wi in range(2):
        out = jnp.dot(both, joined(w_refs, wi), preferred_element_type=F32).astype(BF16)
        for seq in range(n_seqs):
            e_ref[wi, seq] = out[seq * nb:(seq + 1) * nb]
            b_refs[seq][wi, 0] = out[rows + seq * nb:rows + (seq + 1) * nb]


def rest_kernel(n_seqs, x_hbm, *refs):
    w_refs, wq_ref, refs = refs[:2 * PARTS], refs[2 * PARTS], refs[2 * PARTS + 1:]
    g_refs, r_ref, wq_out, (x_scr, sems) = refs[:n_seqs], refs[n_seqs], refs[n_seqs + 1], refs[n_seqs + 2:]
    rows = x_scr.shape[0] // 8
    nb = rows // n_seqs
    own = pl.program_id(0)

    @pl.when(own == 0)
    def _():
        for slot in (2, 3, 4, 5, 6, 7, 0, 1):
            slot_copy(x_hbm, x_scr, sems, slot).start()
        for slot in range(2, 8):
            slot_copy(x_hbm, x_scr, sems, slot).wait()

    @pl.when(own == 2)
    def _():
        for slot in range(2):
            slot_copy(x_hbm, x_scr, sems, slot).wait()

    split_block(onehot(), (wq_ref,), wq_out, tuple(range(8)))
    pair = pl.ds(pl.multiple_of((own // 2 + 1 - 2 * (own // 2 % 2)) * 2 * rows, 2 * rows), 2 * rows)
    half = pl.ds(pl.multiple_of((1 - own // 4) * 4 * rows, 4 * rows), 4 * rows)
    for wi in range(2):
        weight = joined(w_refs, wi)
        out = jnp.dot(x_scr[pair, :], weight, preferred_element_type=F32).astype(BF16)
        for slot in range(2):
            for seq in range(n_seqs):
                at = (slot * n_seqs + seq) * nb
                g_refs[seq][wi, 0, slot * nb:(slot + 1) * nb, :] = out[at:at + nb]
        out = jnp.dot(x_scr[half, :], weight, preferred_element_type=F32).astype(BF16)
        for slot in range(4):
            for seq in range(n_seqs):
                at = (slot * n_seqs + seq) * nb
                r_ref[wi, seq, slot * nb:(slot + 1) * nb, :] = out[at:at + nb]


def query_kernel(n_seqs, x_hbm, *refs):
    w_refs, q_ref, refs = refs[:PARTS], refs[PARTS], refs[PARTS + 1:]
    first_refs, (x_scr, sems) = refs[:n_seqs], refs[n_seqs:]
    rows = x_scr.shape[0] // 8
    nb = rows // n_seqs
    own = pl.program_id(0)

    @pl.when(own == 0)
    def _():
        for slot in range(8):
            slot_copy(x_hbm, x_scr, sems, slot).start()
        for slot in range(8):
            slot_copy(x_hbm, x_scr, sems, slot).wait()

    out = jnp.dot(x_scr[...], joined(w_refs, 0), preferred_element_type=F32).astype(BF16)
    for slot in range(8):
        far_pos = jnp.where(slot // 4 == own // 4, 2 + slot % 2, 4 + slot % 4)
        pos = jnp.where(slot == own, 0, jnp.where(slot // 2 == own // 2, 1, far_pos))
        for seq in range(n_seqs):
            at = (slot * n_seqs + seq) * nb
            q_ref[0, seq, pl.ds(pl.multiple_of(pos * nb, nb), nb), :] = out[at:at + nb]
    for seq in range(n_seqs):
        first_refs[seq][0, 0] = q_ref[0, seq, :nb, :]


def w_spec(block, part):
    return pl.BlockSpec(block, lambda g: (swap_bits(g), part, 0))


def project(kernel, xp, ws, n_seqs, outs, natural=None):
    n_heads, model_dim, head_dim = ws[0].shape
    out_rows = sum(n_w * seqs * n for n_w, seqs, n in outs)
    out_specs = [pl.BlockSpec((n_w, seqs, None, n, head_dim), lambda g: (0, 0, swap_bits(g), 0, 0)) for n_w, seqs, n in outs]
    out_shape = [jax.ShapeDtypeStruct((n_w, seqs, n_heads, n, head_dim), BF16) for n_w, seqs, n in outs]
    in_specs = [pl.BlockSpec(memory_space=pl.ANY)]
    in_specs += [w_spec((1, model_dim // PARTS, head_dim), part) for _ in ws for part in range(PARTS)]
    more = ()
    if natural is not None:
        more = (natural,)
        in_specs.append(pl.BlockSpec((natural.shape[0] // n_heads, head_dim), lambda g: (g, 0)))
        out_specs.append(pl.BlockSpec((8, model_dim // n_heads, head_dim), lambda g: (0, g, 0)))
        out_shape.append(jax.ShapeDtypeStruct((8, model_dim, head_dim), BF16))
    return pl.pallas_call(
        functools.partial(kernel, n_seqs),
        grid=(n_heads,),
        in_specs=in_specs,
        out_specs=out_specs,
        out_shape=out_shape,
        scratch_shapes=[pltpu.VMEM(xp.shape, BF16), pltpu.SemaphoreType.DMA((8,))],
        cost_estimate=cost(2 * n_heads * out_rows * model_dim * head_dim, 2 * (xp.size + len(ws) * ws[0].size) + 2 * n_heads * out_rows * head_dim),
        name="project",
    )(xp, *[w for w in ws for _ in range(PARTS)], *more)


def mult_of(group, key_group, level):
    return min(group, key_group) - level + 1


def by_group(groups, key_group, level, log=False):
    mults = [mult_of(group, key_group, level) for group, _ in groups]
    if all(mult == 1 for mult in mults):
        return None
    values = [math.log2(mult) if log else float(mult) for mult in mults]
    n_cols = sum(cols for _, cols in groups)
    col = lax.broadcasted_iota(jnp.int32, (1, n_cols), 1)
    row, base = jnp.full((1, n_cols), values[-1], F32), n_cols
    for value, (_, cols) in list(zip(values, groups))[::-1]:
        row = jnp.where(col < base, value, row)
        base -= cols
    return row


def scores(keys, q):
    return lax.dot_general(keys, q, (((1,), (1,)), ((), ())), preferred_element_type=F32)


def fold(op, p):
    return op(p.reshape(p.shape[0] // 8, 8, p.shape[1]), axis=0)


def gather_keys(kv_refs, k_scr, v_scr):
    off = 0
    for ref in kv_refs:
        rows = ref.shape[1]
        k_scr[off:off + rows, :] = ref[0]
        v_scr[:, off:off + rows] = jnp.transpose(ref[1])
        off += rows


def branch0_stages(q, k_scr, v_scr, segs, step, groups, s_scr, p_scr, result):
    scale = LOG2E * q.shape[1] ** -0.5
    peak = None
    for start in range(0, k_scr.shape[0], step):
        s = scores(k_scr[start:start + step, :], q)
        s_scr[start:start + step, :] = s
        top = fold(jnp.max, s)
        peak = top if peak is None else jnp.maximum(peak, top)
        yield
    shift = jnp.max(peak, axis=0, keepdims=True) * scale
    sums, start = [], 0
    for length, _ in segs:
        p = jnp.exp2(s_scr[start:start + length, :] * scale - shift)
        s_scr[start:start + length, :] = p
        sums.append(jnp.sum(fold(jnp.sum, p), axis=0, keepdims=True))
        start += length
        yield
    total = functools.reduce(jnp.add, sums)
    inverse = 1.0 / total
    weight, start = None, 0
    for (length, key_group), part in zip(segs, sums):
        mult = by_group(groups, key_group, 0)
        factor = inverse if mult is None else inverse * mult
        p_scr[start:start + length, :] = (s_scr[start:start + length, :] * factor).astype(BF16)
        weight = part * factor if weight is None else weight + part * factor
        start += length
        yield
    acc = jnp.dot(v_scr[...], p_scr[...], preferred_element_type=F32)
    result.extend((shift + jnp.log2(total), weight, acc))
    yield


def level0_kernel(nb, q_ref, *refs):
    kv_refs, (o_ref, acc_ref, stat_ref, k_scr, v_scr, s_scr, p_scr, s_scr2, p_scr2) = refs[:8], refs[8:]
    gather_keys(kv_refs, k_scr, v_scr)
    segs = ((2 * nb, 3), (2 * nb, 2), (4 * nb, 1), (4 * nb, 0), (4 * nb, 0))
    groups = ((3, nb), (2, nb), (1, 2 * nb))
    high, low = [], []
    lead = branch0_stages(q_ref[4 * nb:, :], k_scr, v_scr, segs, 4 * nb, ((0, 4 * nb),), s_scr2, p_scr2, high)
    trail = branch0_stages(q_ref[:4 * nb, :], k_scr, v_scr, segs, 4 * nb, groups, s_scr, p_scr, low)
    for _ in range(4):
        next(lead)
    while not low:
        next(lead, None)
        next(trail)
    shift, weight, acc = low
    acc_ref[...] = acc
    stat_ref[0:1, :] = shift
    stat_ref[1:2, :] = weight
    o_ref[...] = jnp.transpose(high[2]).astype(BF16)


def weights(s, shift, scale, segs, groups, level, p_scr):
    start, total = 0, None
    for length, key_group in segs:
        mult = by_group(groups, key_group, level, log=True)
        local = shift if mult is None else shift - mult
        p = jnp.exp2(s[start:start + length, :] * scale - local)
        p_scr[start:start + length, :] = p.astype(BF16)
        part = fold(jnp.sum, p)
        total = part if total is None else total + part
        start += length
    return jnp.sum(total, axis=0, keepdims=True)


def peak_of(s, scale):
    return jnp.max(fold(jnp.max, s), axis=0, keepdims=True) * scale


def upper(op, low, row):
    n_cols = low.shape[1]
    return jnp.concatenate([op(row[:, :n_cols], low), row[:, n_cols:]], axis=1)


def level1_kernel(nb, q_ref, *refs):
    kv_refs, (acc_in, stat_in, o_ref, acc_ref, stat_ref, k_scr, v_scr, p_scr) = refs[:6], refs[6:]
    gather_keys(kv_refs, k_scr, v_scr)
    scale = LOG2E * q_ref.shape[1] ** -0.5
    s = scores(k_scr[...], q_ref[...])
    shift_near, sum_near = stat_in[0:1, :], stat_in[1:2, :]
    shift = jnp.maximum(shift_near, peak_of(s, scale))
    total = weights(s, shift, scale, ((2 * nb, 3), (2 * nb, 2), (4 * nb, 1)), ((3, nb), (2, nb), (1, 2 * nb)), 1, p_scr)
    near_scale = jnp.exp2(shift_near - shift)
    total = sum_near * near_scale + total
    acc = acc_in[...] * near_scale + jnp.dot(v_scr[...], p_scr[...], preferred_element_type=F32)
    acc_ref[...] = acc[:, :2 * nb]
    stat_ref[0:1, :] = shift[:, :2 * nb]
    stat_ref[1:2, :] = total[:, :2 * nb]
    o_ref[...] = jnp.transpose(acc[:, 2 * nb:] * (1.0 / total[:, 2 * nb:])).astype(BF16)


def level2_kernel(nb, q_ref, *refs):
    kv_refs, (acc_in, stat_in, far_ref, o_ref, k_scr, v_scr, p_scr) = refs[:8], refs[8:]
    gather_keys(kv_refs, k_scr, v_scr)
    head_dim = q_ref.shape[1]
    scale = LOG2E * head_dim ** -0.5
    s = scores(k_scr[...], q_ref[...])
    shift_near, sum_near = stat_in[0:1, :], stat_in[1:2, :]
    shift_far, sum_far = far_ref[head_dim:head_dim + 1, :], far_ref[head_dim + 1:head_dim + 2, :]
    shift = upper(jnp.maximum, shift_far, jnp.maximum(shift_near, peak_of(s, scale)))
    total = weights(s, shift, scale, ((4 * nb, 3), (4 * nb, 2)), ((3, nb), (2, nb)), 2, p_scr)
    near_scale = jnp.exp2(shift_near - shift)
    far_scale = jnp.exp2(shift_far - shift[:, :nb])
    total = upper(jnp.add, sum_far * far_scale, sum_near * near_scale + total)
    acc = acc_in[...] * near_scale + jnp.dot(v_scr[...], p_scr[...], preferred_element_type=F32)
    acc = upper(jnp.add, far_ref[:head_dim, :] * far_scale, acc)
    o_ref[...] = jnp.transpose(acc * (1.0 / total)).astype(BF16)


def far_kernel(nb, q_ref, *refs):
    kv_refs, (far_ref, k_scr, v_scr, p_scr) = refs[:8], refs[8:]
    gather_keys(kv_refs, k_scr, v_scr)
    head_dim = q_ref.shape[1]
    scale = LOG2E * head_dim ** -0.5
    s = scores(k_scr[...], q_ref[...])
    shift = peak_of(s, scale)
    total = weights(s, shift, scale, ((8 * nb, 3),), ((3, nb),), 3, p_scr)
    far_ref[:head_dim, :] = jnp.dot(v_scr[...], p_scr[...], preferred_element_type=F32)
    far_ref[head_dim:, :] = jnp.concatenate([shift, total] + [jnp.zeros_like(shift)] * 6, axis=0)


def attend(body, nb, q, q_rows, kvs, states, outs, seq, scratch, pairs):
    n_heads, head_dim = q.shape[2], q.shape[4]
    n_keys = sum(kv.shape[3] for kv in kvs)

    def spec(n_here, *dims):
        base = seq if n_here > 1 else 0
        return pl.BlockSpec((None, None, *dims), lambda h: (base, h, 0, 0))

    def lead_spec(lead, n_here, rows):
        base = seq if n_here > 1 else 0
        return pl.BlockSpec((lead, None, None, rows, head_dim), lambda h: (0, base, h, 0, 0))

    return pl.pallas_call(
        functools.partial(body, nb),
        grid=(n_heads,),
        in_specs=[lead_spec(None, q.shape[1], q_rows)]
        + [lead_spec(2, kv.shape[1], kv.shape[3]) for kv in kvs]
        + [spec(state.shape[0], *state.shape[2:]) for state in states],
        out_specs=[spec(1, rows, width) for rows, width, _ in outs],
        out_shape=[jax.ShapeDtypeStruct((1, n_heads, rows, width), dtype) for rows, width, dtype in outs],
        scratch_shapes=[pltpu.VMEM(dims, dtype) for dims, dtype in scratch],
        cost_estimate=cost(4 * n_heads * pairs * head_dim, 2 * n_heads * head_dim * (q_rows + 2 * n_keys), n_heads * pairs),
    )(q, *kvs, *states)


def out_kernel(nb, o_low, o_mid, o_high, w_ref, *refs):
    y_ref, mix, lhs = refs[-3:]
    n_tok = lhs.shape[0]

    @pl.when(pl.program_id(0) == 0)
    def _():
        back = onehot(transposed=True)
        for sub in range(n_tok // TILE):
            for res in range(8):
                for head in range(8):
                    pos = position(SLOT[res], SLOT[head])
                    ref, base = (o_low, 0) if pos < 2 else (o_mid, 2) if pos < 4 else (o_high, 4)
                    first = (pos - base) * nb + sub * 32
                    piece = ref[0, head, first:first + 32, :]
                    mix[res * 32:(res + 1) * 32, head * piece.shape[1]:(head + 1) * piece.shape[1]] = piece
            lhs[sub * TILE:(sub + 1) * TILE, :] = jnp.dot(back, mix[...], preferred_element_type=F32).astype(BF16)

    y_ref[0] = jnp.dot(lhs[...], w_ref[...], preferred_element_type=F32).astype(BF16)


def out_project(o_low, o_mid, o_high, w, nb, seq, n_seqs, y_prev):
    width, model_dim = w.shape
    n_tok = nb * 8
    n_cols = min(512, model_dim)
    in_specs = [pl.BlockSpec(a.shape, lambda i: (0, 0, 0, 0)) for a in (o_low, o_mid, o_high)] + [pl.BlockSpec((width, n_cols), lambda i: (0, i))]
    more = () if y_prev is None else (y_prev,)
    return pl.pallas_call(
        functools.partial(out_kernel, nb),
        grid=(model_dim // n_cols,),
        in_specs=in_specs + [pl.BlockSpec(memory_space=pl.ANY) for _ in more],
        out_specs=pl.BlockSpec((1, n_tok, n_cols), lambda i: (seq, 0, i)),
        out_shape=jax.ShapeDtypeStruct((n_seqs, n_tok, model_dim), BF16),
        scratch_shapes=[pltpu.VMEM((TILE, width), BF16), pltpu.VMEM((n_tok, width), BF16)],
        input_output_aliases={4: 0} if more else {},
        cost_estimate=cost(2 * n_tok * width * model_dim, 4 * n_tok * width + 2 * w.size),
        name="out_project",
    )(o_low, o_mid, o_high, w, *more)


def solution(mesh):
    n_dev = mesh.shape['sp']

    def swap(a, bit):
        return lax.ppermute(a, 'sp', [(d, d ^ bit) for d in range(n_dev)])

    def local_step(x_loc, w_q, w_k, w_v, w_o):
        n_seqs, n_tok, model_dim = x_loc.shape
        n_heads, head_dim = w_q.shape[1], w_q.shape[2]
        nb = n_tok // 8
        n_rows = n_seqs * n_tok
        after = lax.optimization_barrier

        seqs = range(n_seqs)
        natural = [w.reshape(model_dim * n_heads, head_dim) for w in (w_q, w_k, w_v)]
        plain = tuple(range(8))
        xp, wk, wv = split_rows((x_loc.reshape(n_rows, model_dim), *natural[1:]), (SLOT, plain, plain), 2 if n_rows < 8 * TILE else 8)
        xp = xp.reshape(n_rows, model_dim)

        e, *b = project(near_kernel, xp, (wk, wv), n_seqs, ((2, n_seqs, nb),) + ((2, 1, nb),) * n_seqs)
        wk, wv, e, b = after((wk, wv, e, b))
        y_e, z_e, c_e = swap(e, 2), swap(e, 4), swap(e, 1)
        y_b, c_b = [swap(b[seq], 2) for seq in seqs], [swap(b[seq], 1) for seq in seqs]
        *g, r, wq = project(rest_kernel, xp, (wk, wv), n_seqs, ((2, 1, 2 * nb),) * n_seqs + ((2, n_seqs, 4 * nb),), natural[0])
        wq, g, r = after((wq, g, r))
        y_g, c_g = [swap(g[seq], 2) for seq in seqs], [swap(g[seq], 1) for seq in seqs]
        c_r = swap(r, 1)
        q_all, *q_first = project(query_kernel, xp, (wq,), n_seqs, ((1, n_seqs, 8 * nb),) + ((1, 1, nb),) * n_seqs)

        q_all, q_first, y_e, z_e, b_late = after((q_all, q_first, y_e, z_e, b))
        q_far = [swap(q_first[seq], 8) for seq in seqs]
        zy_e, yc_e, zc_e = swap(y_e, 4), swap(y_e, 1), swap(z_e, 1)
        z_b = [swap(b_late[seq], 4) for seq in seqs]

        near = []
        for seq in seqs:
            kvs = (e, c_e, b[seq], c_b[seq], g[seq], c_g[seq], r, c_r)
            keys = 16 * nb
            scratch = [((keys, head_dim), BF16), ((head_dim, keys), BF16)] + [((keys, 4 * nb), F32), ((keys, 4 * nb), BF16)] * 2
            near.append(attend(level0_kernel, nb, q_all, 8 * nb, kvs, (),
                               ((4 * nb, head_dim, BF16), (head_dim, 4 * nb, F32), (8, 4 * nb, F32)), seq, scratch, 8 * nb * keys))
            near[seq], q_all = after((near[seq], q_all))
        near, q_all, q_far, zy_e, y_b = after((near, q_all, q_far, zy_e, y_b))
        zyc_e = swap(zy_e, 1)
        yc_b = [swap(y_b[seq], 1) for seq in seqs]
        far_in = []
        for seq in seqs:
            kvs = (e, c_e, y_e, yc_e, z_e, zc_e, zy_e, zyc_e)
            scratch = [((8 * nb, head_dim), BF16), ((head_dim, 8 * nb), BF16), ((8 * nb, nb), BF16)]
            far, = attend(far_kernel, nb, q_far[seq], nb, kvs, (), ((head_dim + 8, nb, F32),), seq, scratch, 8 * nb * nb)
            far_in.append(swap(far, 8))
        zy_b, zc_b, yc_g, one, token = [], [], [], [], far
        for seq in seqs:
            token, z_b[seq], y_g[seq], q_all = after((token, z_b[seq], y_g[seq], q_all))
            zy_b.append(swap(z_b[seq], 2))
            zc_b.append(swap(z_b[seq], 1))
            yc_g.append(swap(y_g[seq], 1))
            kvs = (y_e, yc_e, y_b[seq], yc_b[seq], y_g[seq], yc_g[seq])
            scratch = [((8 * nb, head_dim), BF16), ((head_dim, 8 * nb), BF16), ((8 * nb, 4 * nb), BF16)]
            one.append(attend(level1_kernel, nb, q_all, 4 * nb, kvs, near[seq][1:],
                              ((2 * nb, head_dim, BF16), (head_dim, 2 * nb, F32), (8, 2 * nb, F32)), seq, scratch, 8 * nb * 4 * nb))
            token = one[seq][2]
        y = None
        w_out = w_o.reshape(n_heads * head_dim, model_dim)
        zyc_b = []
        for seq in seqs:
            token, zy_b[seq] = after((token, zy_b[seq]))
            zyc_b.append(swap(zy_b[seq], 1))
            if seq > 0:
                y = out_project(o_low, one[seq - 1][0], near[seq - 1][0], w_out, nb, seq - 1, n_seqs, y)
            kvs = (z_e, zc_e, zy_e, zyc_e, z_b[seq], zc_b[seq], zy_b[seq], zyc_b[seq])
            scratch = [((8 * nb, head_dim), BF16), ((head_dim, 8 * nb), BF16), ((8 * nb, 2 * nb), BF16)]
            o_low, = attend(level2_kernel, nb, q_all, 2 * nb, kvs, (*one[seq][1:], far_in[seq]), ((2 * nb, head_dim, BF16),), seq,
                            scratch, 8 * nb * 2 * nb)
            token = o_low
        y = out_project(o_low, one[-1][0], near[-1][0], w_out, nb, n_seqs - 1, n_seqs, y)
        return y

    return jax.shard_map(local_step, mesh=mesh, in_specs=(P('dp', 'sp', None), P(), P(), P(), P()), out_specs=P('dp', 'sp', None), check_vma=False)
```
